32 devices in a mesh: batch: 8 (over y, x, core), seq: 4 (over z).
Axes of the slice: x: 2, y: 2, z: 4, core: 2. Of those that a mesh axis runs over, the one named last changes fastest.
Arguments:
- queries: bfloat16 [8, 2048, 1280], P('batch', 'seq'), may hold values from -120 to 120
- keys: bfloat16 [8, 2048, 1280], P('batch', 'seq'), may hold values from -7.5 to 7.5
- values: bfloat16 [8, 2048, 1280], P('batch', 'seq'), may hold values from -6 to 6
- residual_in: bfloat16 [8, 2048, 1280], P('batch', 'seq'), may hold values from -3 to 3
- w_out: bfloat16 [1280, 1280], replicated, may hold values from -0.15625 to 0.15625
- ln_gain: float32 [1280], replicated, may hold values from 0.5 to 1.5
- w_proj: bfloat16 [1280, 1024], replicated, may hold values from -0.15625 to 0.15625
- texts: float32 [8, 1024], P('batch', 'seq'), may hold values from -1200 to 1200
- labels: int32 [8], replicated, may hold values from 0 to 7, each once
Outputs:
- hidden_out: bfloat16 [8, 2048, 1280], P('batch', 'seq')
- image_loss: float32 [8], P('batch')
- text_loss: float32 [8], P('batch')
The draws below stay inside these ranges and needn't reach their ends.
All inputs are finite; a program needn't handle non-finite values.
Results may differ from the reference program's by a relative error of at most 0.0034.
Values may be sent and summed in bfloat16 or wider, within the bound.
A program may use at most 64 MiB of HBM per device.

```python
import jax
import jax.numpy as jnp
from jax import lax

D = 1280
HEADS = 16
HEAD_DIM = 80
EMBED = 1024
PATCHES = 2048
IMAGES = 8
TEXTS = 8


def drawn_pair(key):
    key_query, key_key = jax.random.split(jax.random.fold_in(key, 7), 2)
    shape = (IMAGES, PATCHES, D)
    query_draw = 1.5 * jnp.clip(jax.random.normal(key_query, shape, jnp.float32), -5.0, 5.0)
    key_draw = 1.5 * jnp.clip(jax.random.normal(key_key, shape, jnp.float32), -5.0, 5.0)
    return (query_draw, key_draw)


def draw_queries(key, part):
    return drawn_pair(key)[0].astype(jnp.bfloat16)


def draw_keys(key, part):
    return drawn_pair(key)[1].astype(jnp.bfloat16)


def draw_texts(key, part):
    key_base, key_scale = jax.random.split(jax.random.fold_in(key, 11), 2)
    base = jnp.clip(jax.random.normal(key_base, (TEXTS, EMBED), jnp.float32), -4.5, 4.5)
    scales = jnp.exp(jax.random.uniform(key_scale, (TEXTS, 1), jnp.float32, jnp.log(2.0), jnp.log(20.0)))
    result = base * scales
    return result


def level_of(stream_key, extent, pieces, low, high):
    gain = 1.0
    for axis_at, shards_of in pieces:
        draws = jax.random.uniform(jax.random.fold_in(jax.random.fold_in(stream_key, 6), axis_at), (shards_of,), jnp.float32, low / len(pieces), high / len(pieces))
        gain = gain * jnp.repeat(jnp.exp(draws), extent[axis_at] // shards_of).reshape((-1,) + (1,) * (len(extent) - 1 - axis_at))
    return gain


def scatter_about(stream_key, shape, width, bound, shards=(), kind=jnp.bfloat16):
    values = width * jax.random.normal(stream_key, shape, jnp.float32)
    if shards:
        values = values * level_of(stream_key, shape, shards, -0.22, 0.18)
    return jnp.clip(values, -bound, bound).astype(kind)


def setup_inputs(seed: int = 0) -> dict:
    key_list = jax.random.split(jax.random.key(seed), 10)
    queries = draw_queries(jax.random.fold_in(key_list[9], 71), 0)
    keys = draw_keys(jax.random.fold_in(key_list[9], 71), 0)
    values = scatter_about(key_list[2], (IMAGES, PATCHES, D), 1.0, 6.0, ((0, 8), (1, 4)))
    residual_in = scatter_about(key_list[3], (IMAGES, PATCHES, D), 0.5, 3.0, ((0, 8), (1, 4)))
    w_out = scatter_about(key_list[4], (D, D), D ** -0.5, 0.15625)
    ln_gain = jnp.clip(1.0 + 0.1 * jax.random.normal(key_list[5], (D,), jnp.float32), 0.5, 1.5)
    w_proj = scatter_about(key_list[6], (D, EMBED), D ** -0.5, 0.15625)
    texts = draw_texts(jax.random.fold_in(key_list[9], 71), 0)
    labels = jax.random.permutation(key_list[8], TEXTS).astype(jnp.int32)
    return dict(queries=queries, keys=keys, values=values, residual_in=residual_in, w_out=w_out, ln_gain=ln_gain, w_proj=w_proj, texts=texts, labels=labels)


def attend_image(operands):
    query_rows, key_rows, value_rows = operands
    block_rows = min(512, PATCHES)
    query_heads = query_rows.astype(jnp.float32).reshape(PATCHES, HEADS, HEAD_DIM)
    key_heads = key_rows.astype(jnp.float32).reshape(PATCHES, HEADS, HEAD_DIM)
    value_heads = value_rows.astype(jnp.float32).reshape(PATCHES, HEADS, HEAD_DIM)
    score_scale = HEAD_DIM ** (-0.5)

    def one_block(offset):
        query_block = lax.dynamic_slice_in_dim(query_heads, offset, block_rows, 0)
        scores = jnp.einsum('qhd,khd->hqk', query_block, key_heads) * score_scale
        maxima = lax.optimization_barrier(jnp.max(scores, axis=-1, keepdims=True))
        weights = jnp.exp(scores - maxima)
        weights = (weights / lax.optimization_barrier(jnp.sum(weights, axis=-1, keepdims=True))).astype(jnp.bfloat16)
        weights = lax.optimization_barrier(weights)
        mixed = jnp.einsum('hqk,khd->qhd', weights.astype(jnp.float32), value_heads)
        return mixed.astype(jnp.bfloat16).reshape(block_rows, D)
    offsets = (jnp.arange(PATCHES // block_rows) * block_rows).astype(jnp.int32)
    return lax.map(one_block, offsets).reshape(PATCHES, D)

def row_lse(logits, axis):
    maxima = lax.optimization_barrier(jnp.max(logits, axis=axis, keepdims=True))
    return jnp.squeeze(maxima, axis) + jnp.log(lax.optimization_barrier(jnp.sum(jnp.exp(logits - maxima), axis=axis)))

def contrastive(logits, labels):
    matched = labels[:, None] == jnp.arange(logits.shape[1], dtype=jnp.int32)[None, :]
    picked = jnp.where(matched, logits, jnp.float32(0.0))
    image_loss = row_lse(logits, 1) - lax.optimization_barrier(jnp.sum(picked, axis=1))
    text_loss = row_lse(logits, 0) - lax.optimization_barrier(jnp.sum(picked, axis=0))
    return (image_loss, text_loss)

def reference(queries, keys, values, residual_in, w_out, ln_gain, w_proj, texts, labels):
    attended = lax.map(attend_image, (queries, keys, values))
    mixed_out = jnp.dot(attended.reshape(-1, D), w_out, preferred_element_type=jnp.float32)
    summed = residual_in.astype(jnp.float32) + mixed_out.reshape(IMAGES, PATCHES, D)
    hidden_out = summed.astype(jnp.bfloat16)
    centred = summed - lax.optimization_barrier(jnp.mean(summed, axis=-1, keepdims=True))
    variance = lax.optimization_barrier(jnp.mean(centred * centred, axis=-1, keepdims=True))
    normed = centred * lax.rsqrt(variance + 1e-05) * ln_gain
    pooled = lax.optimization_barrier(jnp.mean(normed, axis=1))
    embedding = jnp.dot(pooled, w_proj.astype(jnp.float32), precision=lax.Precision.HIGHEST)
    inverse = lax.rsqrt(lax.optimization_barrier(jnp.sum(embedding * embedding, axis=1)) + 1e-06)
    logits = jnp.dot(embedding * inverse[:, None], texts.T, precision=lax.Precision.HIGHEST)
    image_loss, text_loss = contrastive(logits, labels)
    return (hidden_out, image_loss, text_loss)
```

```python
import functools

import jax
import jax.numpy as jnp
from jax import lax
from jax.experimental import pallas as pl
from jax.experimental.pallas import tpu as pltpu
from jax.sharding import PartitionSpec as P

HEADS = 16
HEAD_DIM = 80
EMBED = 1024
LANES = 128
ONES_ROWS = 16
MESH = pl.DeviceIdType.MESH


def fused_kernel(
    nb, nz,
    q_hbm, k_hbm, v_hbm, res_hbm, w_hbm, gain_hbm, wproj_hbm, texts_hbm,
    hid_out, row_out,
    k_in, q_in, v_in, k_t, q_t, v_t, q_all, k_all, v_all, k_rows,
    gain_ref, texts_ref, o_send, att_t, w_v, res_v, acc, hid_v, wproj_v, text_all, pool_all, row_all,
    in_sem, load_sem, move_send, move_recv, o_ssem, o_rsem,
    text_ssem, text_rsem, wide_ssem, wide_rsem, pool_ssem, pool_rsem, row_ssem, row_rsem, hid_sem,
):
    b = lax.axis_index("batch")
    z = lax.axis_index("seq")
    tok, features = q_in.shape
    local = HEADS // nz
    cols = texts_ref.shape[1]
    half = max(1, nz // 2)
    ends = [-(-(j + 1) * nz * HEAD_DIM // LANES) * LANES for j in range(local)]
    groups = list(zip([0] + ends[:-1], ends))

    def partner(t):
        side = lax.rem(z // half + (1 if t < nz - half else 0), nz // half)
        return side * half + lax.rem(z + t + 1, half)

    barrier = pltpu.get_barrier_semaphore()
    sources, held, turned = (k_hbm, q_hbm, v_hbm), (k_in, q_in, v_in), (k_t, q_t, v_t)

    def in_copy(arr, j):
        at = pl.ds(groups[j][0], groups[j][1] - groups[j][0])
        return pltpu.make_async_copy(
            sources[arr].at[0, :, at], held[arr].at[:, at], in_sem.at[arr, j]
        )

    for t in range(nz - 1):
        pl.semaphore_signal(
            barrier, inc=1, device_id={"seq": partner(t)}, device_id_type=MESH
        )
    for j in range(local):
        for arr in range(3):
            in_copy(arr, j).start()
    for r in range(1, nb):
        pl.semaphore_signal(
            barrier, inc=1, device_id={"batch": lax.rem(b + r, nb)}, device_id_type=MESH
        )
    loads = [
        pltpu.make_async_copy(src, dst, load_sem.at[i])
        for i, (src, dst) in enumerate(
            (
                (res_hbm.at[0], res_v), (wproj_hbm, wproj_v), (w_hbm, w_v),
                (gain_hbm, gain_ref),
            )
        )
    ]
    text_load = pltpu.make_async_copy(texts_hbm, texts_ref, load_sem.at[4])
    text_load.start()
    for copy in loads:
        copy.start()

    v_all[:, :, pl.ds(HEAD_DIM, ONES_ROWS), :] = jnp.ones(
        (local, nz, ONES_ROWS, tok), jnp.bfloat16
    )

    def turn(arr, j):
        in_copy(arr, j).wait()
        for at in range(groups[j][0], groups[j][1], LANES):
            turned[arr][pl.ds(at, LANES), :] = held[arr][:, pl.ds(at, LANES)].T

    def piece(arr, j, src):
        return (k_all, q_all, v_all)[arr].at[j, src, pl.ds(0, HEAD_DIM), :]

    def rows_of(arr, j, dst):
        at = pl.multiple_of((j * nz + dst) * HEAD_DIM, 16)
        return turned[arr].at[pl.ds(at, HEAD_DIM), :]

    def remote(arr, j, t):
        dst = partner(t)
        return pltpu.make_async_remote_copy(
            src_ref=rows_of(arr, j, dst),
            dst_ref=piece(arr, j, z),
            send_sem=move_send.at[arr],
            recv_sem=move_recv.at[arr, j],
            device_id={"seq": dst},
            device_id_type=MESH,
        )

    def send_piece(arr, j):
        for t in range(nz - 1):
            remote(arr, j, t).start()
        pltpu.make_async_copy(rows_of(arr, j, z), piece(arr, j, z), move_recv.at[arr, j]).start()

    def text_copy(t):
        return pltpu.make_async_remote_copy(
            src_ref=texts_ref,
            dst_ref=text_all.at[b, z],
            send_sem=text_ssem,
            recv_sem=text_rsem,
            device_id={"seq": partner(t)},
            device_id_type=MESH,
        )

    def wide_copy(r):
        return pltpu.make_async_remote_copy(
            src_ref=text_all.at[b],
            dst_ref=text_all.at[b],
            send_sem=wide_ssem,
            recv_sem=wide_rsem,
            device_id={"batch": lax.rem(b + r, nb)},
            device_id_type=MESH,
        )

    def await_bytes(ref, sem):
        pltpu.make_async_copy(ref, ref, sem).wait()

    for j in range(local):
        for arr in range(3):
            turn(arr, j)
            if j == arr == 0:
                pl.semaphore_wait(barrier, nz - 1 + nb - 1)
            send_piece(arr, j)
            if j == arr == 0:
                text_load.wait()
                for t in range(nz - 1):
                    text_copy(t).start()
                text_all[b, z] = texts_ref[...]

    row_block = min(128, tok)
    chunks = tok // row_block

    def o_rows(j, src, c):
        at = pl.multiple_of(src * HEAD_DIM, 16)
        return att_t.at[j, pl.ds(at, HEAD_DIM), pl.ds(c * row_block, row_block)]

    def o_copy(j, t, c):
        dst = partner(t)
        return pltpu.make_async_remote_copy(
            src_ref=o_send.at[j, dst, :, pl.ds(c * row_block, row_block)],
            dst_ref=o_rows(j, z, c),
            send_sem=o_ssem,
            recv_sem=o_rsem.at[j, c],
            device_id={"seq": dst},
            device_id_type=MESH,
        )

    def o_arrive(j, c):
        here = pl.ds(c * row_block, row_block)
        await_bytes(att_t.at[j, pl.ds(0, (nz - 1) * HEAD_DIM), here], o_rsem.at[j, c])

    far = nz - half
    scale = HEAD_DIM ** (-0.5) * 1.4426950408889634

    def arrive(arr, j):
        ref = (k_all, q_all, v_all)[arr].at[j, :, pl.ds(0, HEAD_DIM), :]
        await_bytes(ref, move_recv.at[arr, j])

    def partner_at(t):
        crossing = jnp.where(t < nz - half, 1, 0)
        side = lax.rem(z // half + crossing, nz // half)
        return side * half + lax.rem(z + t + 1, half)

    def attend(index, carry):
        j = index // nz
        t = lax.rem(index, nz)

        @pl.when(t == 0)
        def _():
            arrive(0, j)
            for src in range(nz):
                k_rows[pl.ds(src * tok, tok), :] = k_all[j, src].T
            arrive(1, j)

        dst = partner_at(t)
        s = jnp.dot(k_rows[...], q_all[j, dst], preferred_element_type=jnp.float32)
        p = jnp.exp2((s - jnp.max(s, axis=0, keepdims=True)) * scale).astype(jnp.bfloat16)

        @pl.when(t == 0)
        def _():
            arrive(2, j)

        out = jnp.zeros((HEAD_DIM + ONES_ROWS, tok), jnp.float32)
        for src in range(nz):
            out += jnp.dot(
                v_all[j, src], p[src * tok:(src + 1) * tok], preferred_element_type=jnp.float32
            )
        mixed = (out[:HEAD_DIM] / out[HEAD_DIM:HEAD_DIM + 1]).astype(jnp.bfloat16)

        for at in range(nz - 1):

            @pl.when(t == at)
            def _():
                o_send[j, partner(at)] = mixed

                @pl.when((j < local - 1) | (at >= far))
                def _():
                    for c in range(chunks):
                        o_copy(j, at, c).start()

                if at == far - 1:

                    @pl.when(j == local - 1)
                    def _():
                        for c in range(chunks):
                            for near in range(far):
                                o_copy(j, near, c).start()

        @pl.when(t == nz - 1)
        def _():
            att_t[j, pl.ds(pl.multiple_of(z * HEAD_DIM, 16), HEAD_DIM), :] = mixed

        @pl.when((j == 0) & (t == nz - 1))
        def _():
            await_bytes(text_all.at[b, pl.ds(0, nz - 1)], text_rsem)
            for r in range(1, nb):
                wide_copy(r).start()

        return carry

    lax.fori_loop(0, local * nz, attend, 0)

    for copy in loads:
        copy.wait()
    depth = nz * HEAD_DIM

    def product(j, c):
        return jnp.dot(
            att_t[j, :, pl.ds(c * row_block, row_block)].T,
            w_v[pl.ds(j * depth, depth), :],
            preferred_element_type=jnp.float32,
        )

    for j in range(local - 1):
        for c in range(chunks):
            here = pl.ds(c * row_block, row_block)
            o_arrive(j, c)
            old = res_v[here, :].astype(jnp.float32) if j == 0 else acc[here, :]
            acc[here, :] = old + product(j, c)
    await_bytes(text_all.at[pl.ds(0, nb - 1)], wide_rsem)

    pool = jnp.zeros((1, features), jnp.float32)
    for c in range(chunks):
        here = pl.ds(c * row_block, row_block)
        o_arrive(local - 1, c)
        old = res_v[here, :].astype(jnp.float32) if local == 1 else acc[here, :]
        summed = old + product(local - 1, c)
        hid_v[here, :] = summed.astype(jnp.bfloat16)
        pltpu.make_async_copy(hid_v.at[here, :], hid_out.at[0, here, :], hid_sem).start()
        centred = summed - jnp.mean(summed, axis=-1, keepdims=True)
        variance = jnp.mean(centred * centred, axis=-1, keepdims=True)
        pool += jnp.sum(centred * lax.rsqrt(variance + 1e-05), axis=0, keepdims=True)

    pool_all[z] = pool * gain_ref[...].reshape(1, features)

    def pool_copy(t):
        return pltpu.make_async_remote_copy(
            src_ref=pool_all.at[z],
            dst_ref=pool_all.at[z],
            send_sem=pool_ssem,
            recv_sem=pool_rsem,
            device_id={"seq": partner(t)},
            device_id_type=MESH,
        )

    for t in range(nz - 1):
        pool_copy(t).start()
    await_bytes(pool_all.at[pl.ds(0, nz - 1)], pool_rsem)
    pooled = pool_all[0]
    for src in range(1, nz):
        pooled = pooled + pool_all[src]
    pooled = pooled / (nz * tok)

    high = pooled.astype(jnp.bfloat16).astype(jnp.float32)
    middle = (pooled - high).astype(jnp.bfloat16).astype(jnp.float32)
    low = pooled - high - middle
    row_id = lax.broadcasted_iota(jnp.int32, (16, features), 0)
    parts = jnp.where(
        row_id == 0, high, jnp.where(row_id == 1, middle, jnp.where(row_id == 2, low, 0.0))
    ).astype(jnp.bfloat16)
    embed = jnp.sum(
        jnp.dot(parts, wproj_v[...], preferred_element_type=jnp.float32), axis=0, keepdims=True
    )
    products = jnp.zeros((nb, 1), jnp.float32)
    for src in range(nz):
        texts = text_all[:, src].reshape(nb, cols)
        products += jnp.sum(
            texts * embed[:, src * cols:(src + 1) * cols], axis=1, keepdims=True
        )
    squares = jnp.sum(embed * embed, axis=1, keepdims=True)
    rows = lax.broadcasted_iota(jnp.int32, (nb, LANES), 0)
    lanes = lax.broadcasted_iota(jnp.int32, (nb, LANES), 1)
    row = jnp.sum(jnp.where(rows == lanes, products, 0.0), axis=0, keepdims=True)
    row_all[b] = jnp.where(lanes[:1] == nb, squares, row)

    def row_copy(r):
        return pltpu.make_async_remote_copy(
            src_ref=row_all.at[b],
            dst_ref=row_all.at[b],
            send_sem=row_ssem,
            recv_sem=row_rsem,
            device_id={"batch": lax.rem(b + r, nb)},
            device_id_type=MESH,
        )

    for r in range(1, nb):
        row_copy(r).start()

    for arr in range(3):
        await_bytes(k_all.at[:, pl.ds(0, nz - 1)], move_send.at[arr])
    await_bytes(o_send.at[:, pl.ds(0, nz - 1)], o_ssem)
    await_bytes(text_all.at[b, pl.ds(0, nz - 1)], text_ssem)
    await_bytes(text_all.at[pl.ds(0, nb - 1)], wide_ssem)
    await_bytes(pool_all.at[pl.ds(0, nz - 1)], pool_ssem)
    pltpu.make_async_copy(hid_v, hid_out.at[0], hid_sem).wait()
    await_bytes(row_all.at[pl.ds(0, nb - 1)], row_rsem)
    row_out[...] = row_all[...].reshape(nb, LANES)
    await_bytes(row_all.at[pl.ds(0, nb - 1)], row_ssem)


def loss_kernel(nb, hid_ref, row_ref, labels_ref, hid_out, img_ref, txt_ref, sem):
    store = pltpu.make_async_copy(hid_ref, hid_out, sem)
    store.start()
    b = lax.axis_index("batch")
    rows = lax.broadcasted_iota(jnp.int32, (nb, LANES), 0)
    lanes = lax.broadcasted_iota(jnp.int32, (nb, LANES), 1)
    total = row_ref[...]
    norm = jnp.sum(jnp.where(lanes == nb, total, 0.0), axis=1, keepdims=True)
    logits = total * lax.rsqrt(norm + 1e-06)
    valid = lanes < nb
    matching = jnp.zeros((nb, LANES), jnp.int32)
    for i in range(nb):
        matching = jnp.where(rows == i, labels_ref[i], matching)
    picked = jnp.where(matching == lanes, logits, 0.0)
    shown = jnp.where(valid, logits, -3e38)
    top = jnp.max(shown, axis=1, keepdims=True)
    image = (
        top
        + jnp.log(jnp.sum(jnp.where(valid, jnp.exp(shown - top), 0.0), axis=1, keepdims=True))
        - jnp.sum(jnp.where(valid, picked, 0.0), axis=1, keepdims=True)
    )
    peak = jnp.max(logits, axis=0, keepdims=True)
    text = (
        peak
        + jnp.log(jnp.sum(jnp.exp(logits - peak), axis=0, keepdims=True))
        - jnp.sum(picked, axis=0, keepdims=True)
    )
    img_ref[0] = jnp.sum(jnp.where((rows == b) & (lanes == 0), image, 0.0))
    txt_ref[0] = jnp.sum(jnp.where((rows == 0) & (lanes == b), text, 0.0))
    store.wait()


def fused(queries, keys, values, residual_in, w_out, ln_gain, w_proj, texts, labels):
    nb, nz = lax.axis_size("batch"), lax.axis_size("seq")
    _, tok, features = queries.shape
    local = HEADS // nz
    chunks = tok // min(128, tok)
    cols = texts.shape[1]
    bf16, f32 = jnp.bfloat16, jnp.float32
    anywhere = pl.BlockSpec(memory_space=pl.ANY)
    smem = pl.BlockSpec(memory_space=pltpu.SMEM)
    dma = pltpu.SemaphoreType.DMA
    wide = pltpu.VMEM((tok, features), bf16)
    tall = pltpu.VMEM((features, tok), bf16)
    hidden_shape = jax.ShapeDtypeStruct((1, tok, features), bf16)
    hidden, rows = pl.pallas_call(
        functools.partial(fused_kernel, nb, nz),
        out_shape=(hidden_shape, jax.ShapeDtypeStruct((nb, LANES), f32)),
        in_specs=[pl.BlockSpec(memory_space=pltpu.HBM)] * 8,
        out_specs=(anywhere, pl.BlockSpec(memory_space=pltpu.VMEM)),
        scratch_shapes=[
            wide, wide, wide, tall, tall, tall,
            pltpu.VMEM((local, nz, HEAD_DIM, tok), bf16),
            pltpu.VMEM((local, nz, HEAD_DIM, tok), bf16),
            pltpu.VMEM((local, nz, HEAD_DIM + ONES_ROWS, tok), bf16),
            pltpu.VMEM((nz * tok, HEAD_DIM), bf16),
            pltpu.VMEM((features,), f32),
            pltpu.VMEM((1, cols), f32),
            pltpu.VMEM((local, nz, HEAD_DIM, tok), bf16),
            pltpu.VMEM((local, nz * HEAD_DIM, tok), bf16),
            pltpu.VMEM((features, features), bf16),
            wide,
            pltpu.VMEM((tok, features), f32),
            wide,
            pltpu.VMEM(w_proj.shape, bf16),
            pltpu.VMEM((nb, nz, 1, cols), f32),
            pltpu.VMEM((nz, 1, features), f32),
            pltpu.VMEM((nb, 1, LANES), f32),
            dma((3, local)), dma((5,)),
            dma((3,)), dma((3, local)),
            dma, dma((local, chunks)),
            dma, dma, dma, dma, dma, dma, dma, dma, dma,
        ],
        compiler_params=pltpu.CompilerParams(
            collective_id=0, has_side_effects=True, vmem_limit_bytes=40 * 1024 * 1024
        ),
    )(
        *(pltpu.with_memory_space_constraint(x, pltpu.HBM) for x in (queries, keys, values, residual_in, w_out, ln_gain, w_proj,
        texts))
    )
    return pl.pallas_call(
        functools.partial(loss_kernel, nb),
        out_shape=(
            hidden_shape, jax.ShapeDtypeStruct((1,), f32), jax.ShapeDtypeStruct((1,), f32),
        ),
        in_specs=[anywhere, pl.BlockSpec(memory_space=pltpu.VMEM), smem],
        out_specs=(pl.BlockSpec(memory_space=pltpu.HBM), smem, smem),
        scratch_shapes=[dma],
        compiler_params=pltpu.CompilerParams(vmem_limit_bytes=4 * 1024 * 1024),
    )(hidden, rows, labels)


def row_lse(logits, axis):
    maxima = jnp.max(logits, axis=axis, keepdims=True)
    return jnp.squeeze(maxima, axis) + jnp.log(jnp.sum(jnp.exp(logits - maxima), axis=axis))


def body(queries, keys, values, residual_in, w_out, ln_gain, w_proj, texts, labels):
    seq_count = lax.axis_size("seq")
    images_here, tok_rows, features = queries.shape
    head_count = HEADS // seq_count
    head_cols = head_count * HEAD_DIM
    score_scale = HEAD_DIM ** (-0.5)
    query_all = lax.all_to_all(queries, "seq", split_axis=2, concat_axis=1, tiled=True)
    key_all = lax.all_to_all(keys, "seq", split_axis=2, concat_axis=1, tiled=True)
    value_all = lax.all_to_all(values, "seq", split_axis=2, concat_axis=1, tiled=True)
    items = query_all.shape[0]
    length = query_all.shape[1]
    block_rows = min(512, length)
    query_heads = query_all.reshape(items, length, head_count, HEAD_DIM)
    key_heads = key_all.reshape(items, length, head_count, HEAD_DIM)
    value_heads = value_all.reshape(items, length, head_count, HEAD_DIM)

    def one_block(offset):
        query_block = lax.dynamic_slice_in_dim(query_heads, offset, block_rows, 1)
        scores = (
            jnp.einsum(
                "nqhd,nkhd->nhqk", query_block, key_heads, preferred_element_type=jnp.float32
            )
            * score_scale
        )
        maxima = jnp.max(scores, axis=-1, keepdims=True)
        weights = jnp.exp(scores - maxima)
        weights = (weights / jnp.sum(weights, axis=-1, keepdims=True)).astype(jnp.bfloat16)
        mixed = jnp.einsum(
            "nhqk,nkhd->nqhd", weights, value_heads, preferred_element_type=jnp.float32
        )
        return mixed.astype(jnp.bfloat16).reshape(items, block_rows, head_cols)

    offsets = jnp.arange(length // block_rows) * block_rows
    blocks = lax.map(one_block, offsets)
    attended = jnp.moveaxis(blocks, 0, 1).reshape(items, length, head_cols)
    attended = lax.all_to_all(attended, "seq", split_axis=1, concat_axis=2, tiled=True)
    mixed_out = jnp.dot(attended.reshape(-1, features), w_out, preferred_element_type=jnp.float32)
    summed = residual_in.astype(jnp.float32) + mixed_out.reshape(images_here, tok_rows, features)
    hidden_out = summed.astype(jnp.bfloat16)
    centred = summed - jnp.mean(summed, axis=-1, keepdims=True)
    variance = jnp.mean(centred * centred, axis=-1, keepdims=True)
    normed = centred * lax.rsqrt(variance + 1e-05) * ln_gain
    pool_part = jnp.sum(normed, axis=1) / (tok_rows * seq_count)
    embed_cols = EMBED // seq_count
    pooled = lax.psum(pool_part, "seq")
    embedding = jnp.dot(pooled, w_proj.astype(jnp.float32), precision=lax.Precision.HIGHEST)
    inverse = lax.rsqrt(jnp.sum(embedding * embedding, axis=1) + 1e-06)
    unit_rows = embedding * inverse[:, None]
    embed_piece = lax.dynamic_slice_in_dim(
        unit_rows, lax.axis_index("seq") * embed_cols, embed_cols, 1
    )
    gathered, text_all = (
        lax.all_gather(embed_piece, "batch", axis=0, tiled=True),
        lax.all_gather(texts, "batch", axis=0, tiled=True),
    )
    logit_part = jnp.dot(gathered, text_all.T, precision=lax.Precision.HIGHEST)
    logits = lax.psum(logit_part, "seq")
    matched = labels[:, None] == jnp.arange(logits.shape[1], dtype=jnp.int32)[None, :]
    picked = jnp.where(matched, logits, jnp.float32(0.0))
    image_all = row_lse(logits, 1) - jnp.sum(picked, axis=1)
    text_every = row_lse(logits, 0) - jnp.sum(picked, axis=0)
    first_row = lax.axis_index("batch") * images_here
    image_loss = lax.dynamic_slice_in_dim(image_all, first_row, images_here, 0)
    text_loss = lax.dynamic_slice_in_dim(text_every, first_row, images_here, 0)
    return (hidden_out, image_loss, text_loss)


def program(queries, keys, values, residual_in, w_out, ln_gain, w_proj, texts, labels):
    nb, nz = lax.axis_size("batch"), lax.axis_size("seq")
    fits = (
        queries.shape[0] == 1
        and texts.shape[0] == 1
        and HEADS % nz == 0
        and nz % 2 == 0
        and HEADS * HEAD_DIM % LANES == 0
        and queries.shape[1] % 128 == 0
        and queries.shape[1] <= 512
        and queries.shape[1] * nz <= 2048
        and texts.shape[1] % LANES == 0
        and nb % 8 == 0
        and nb < LANES
    )
    chosen = fused if fits else body
    return chosen(queries, keys, values, residual_in, w_out, ln_gain, w_proj, texts, labels)


def solution(mesh):
    in_specs = (
        P("batch", "seq", None),
        P("batch", "seq", None),
        P("batch", "seq", None),
        P("batch", "seq", None),
        P(),
        P(),
        P(),
        P("batch", "seq"),
        P(),
    )
    out_specs = (P("batch", "seq", None), P("batch"), P("batch"))
    return jax.shard_map(program, mesh=mesh, in_specs=in_specs, out_specs=out_specs, check_vma=False)
```

```python
import functools

import jax
import jax.numpy as jnp
from jax import lax
from jax.experimental import pallas as pl
from jax.experimental.pallas import tpu as pltpu
from jax.sharding import PartitionSpec as P

HEADS = 16
HEAD_DIM = 80
EMBED = 1024
LANES = 128
ONES_ROWS = 16
MESH = pl.DeviceIdType.MESH


def fused_kernel(
    nb, nz,
    q_hbm, k_hbm, v_hbm, res_hbm, w_hbm, gain_hbm, wproj_hbm, texts_hbm, labels_hbm,
    hid_out, row_out, match_out,
    inputs, k_t, q_t, v_t, kq_all, v_all, k_rows,
    gain_ref, texts_ref, labels_ref, o_send, att_t, w_v, res_v, acc, hid_v, wproj_v, text_all, pool_all, row_all,
    in_sem, load_sem, w_sem, move_send, move_recv, o_ssem, o_rsem,
    text_ssem, text_rsem, wide_ssem, wide_rsem, pool_ssem, pool_rsem, row_ssem, row_rsem, hid_sem,
):
    b = lax.axis_index("batch")
    z = lax.axis_index("seq")
    _, tok, features = inputs.shape
    local = HEADS // nz
    cols = texts_ref.shape[1]
    half = max(1, nz // 2)
    ends = [-(-(j + 1) * nz * HEAD_DIM // LANES) * LANES for j in range(local)]
    groups = list(zip([0] + ends[:-1], ends))

    def partner(t):
        side = lax.rem(z // half + (1 if t < nz - half else 0), nz // half)
        return side * half + lax.rem(z + t + 1, half)

    barrier = pltpu.get_barrier_semaphore()
    sources, turned = (k_hbm, q_hbm, v_hbm), (k_t, q_t, v_t)

    def columns(j):
        return pl.ds(groups[j][0], groups[j][1] - groups[j][0])

    def in_copy(arr, j):
        return pltpu.make_async_copy(
            sources[arr].at[0, :, columns(j)],
            inputs.at[arr, :, columns(j)],
            in_sem.at[arr if j == 0 else 2 + j],
        )

    for t in range(nz - 1):
        pl.semaphore_signal(
            barrier, inc=1, device_id={"seq": partner(t)}, device_id_type=MESH
        )
    for j in range(local):
        for arr in range(3):
            in_copy(arr, j).start()
    for r in range(1, nb):
        pl.semaphore_signal(
            barrier, inc=1, device_id={"batch": lax.rem(b + r, nb)}, device_id_type=MESH
        )
    loads = [
        pltpu.make_async_copy(src, dst, load_sem.at[i])
        for i, (src, dst) in enumerate(
            (
                (res_hbm.at[0], res_v), (wproj_hbm, wproj_v), (gain_hbm, gain_ref),
                (labels_hbm, labels_ref),
            )
        )
    ]
    w_rows = []
    for j in range(local):
        for at in range(nz):
            across = lax.rem(at + half, nz)
            src = jnp.where(z < half, nz - 1 - across, across)
            start = pl.multiple_of((j * nz + src) * HEAD_DIM, 16)
            w_rows.append(
                pltpu.make_async_copy(
                    w_hbm.at[pl.ds(start, HEAD_DIM)],
                    w_v.at[pl.ds((j * nz + at) * HEAD_DIM, HEAD_DIM)],
                    w_sem,
                )
            )
    text_load = pltpu.make_async_copy(texts_hbm, texts_ref, load_sem.at[4])
    text_load.start()
    for copy in loads + w_rows:
        copy.start()

    v_all[:, :, pl.ds(HEAD_DIM, ONES_ROWS), :] = jnp.ones(
        (local, nz, ONES_ROWS, tok), jnp.bfloat16
    )

    def await_bytes(ref, sem):
        pltpu.make_async_copy(ref, ref, sem).wait()

    def turn(arr, j):
        if j == 0:
            in_copy(arr, j).wait()
        elif arr == 0:
            await_bytes(inputs.at[:, :, columns(j)], in_sem.at[2 + j])
        for at in range(groups[j][0], groups[j][1], LANES):
            turned[arr][pl.ds(at, LANES), :] = inputs[arr, :, pl.ds(at, LANES)].T

    def piece(arr, j, src):
        if arr == 2:
            return v_all.at[j, src, pl.ds(0, HEAD_DIM), :]
        return kq_all.at[arr, j, src]

    def landed(arr, j):
        return move_recv.at[local + j if arr == 2 else j]

    def rows_of(arr, j, dst):
        at = pl.multiple_of((j * nz + dst) * HEAD_DIM, 16)
        return turned[arr].at[pl.ds(at, HEAD_DIM), :]

    def remote(arr, j, t):
        dst = partner(t)
        return pltpu.make_async_remote_copy(
            src_ref=rows_of(arr, j, dst),
            dst_ref=piece(arr, j, z),
            send_sem=move_send.at[arr // 2],
            recv_sem=landed(arr, j),
            device_id={"seq": dst},
            device_id_type=MESH,
        )

    def send_piece(arr, j):
        for t in range(nz - 1):
            remote(arr, j, t).start()
        pltpu.make_async_copy(rows_of(arr, j, z), piece(arr, j, z), landed(arr, j)).start()

    def text_copy(t):
        return pltpu.make_async_remote_copy(
            src_ref=texts_ref,
            dst_ref=text_all.at[b, z],
            send_sem=text_ssem,
            recv_sem=text_rsem,
            device_id={"seq": partner(t)},
            device_id_type=MESH,
        )

    def wide_copy(r):
        return pltpu.make_async_remote_copy(
            src_ref=text_all.at[b],
            dst_ref=text_all.at[b],
            send_sem=wide_ssem,
            recv_sem=wide_rsem,
            device_id={"batch": lax.rem(b + r, nb)},
            device_id_type=MESH,
        )

    for j in range(local):
        for arr in range(3):
            turn(arr, j)
            if j == arr == 0:
                pl.semaphore_wait(barrier, nz - 1 + nb - 1)
            send_piece(arr, j)
            if j == arr == 0:
                text_load.wait()
                for t in range(nz - 1):
                    text_copy(t).start()
                text_all[b, z] = texts_ref[...]

    row_block = min(128, tok)
    chunks = tok // row_block

    far = nz - half
    last = local - 1
    middle = (z == half - 1) | (z == half)

    def slot(src, dst):
        return lax.rem(jnp.where(dst < half, nz - 1 - src, src) + half, nz)

    def o_copy(j, t, at, sem):
        dst = partner(t)
        rows = pl.ds(pl.multiple_of(slot(z, dst) * HEAD_DIM, 16), HEAD_DIM)
        return pltpu.make_async_remote_copy(
            src_ref=o_send.at[j, dst, :, at],
            dst_ref=att_t.at[j, rows, at],
            send_sem=o_ssem,
            recv_sem=o_rsem.at[sem],
            device_id={"seq": dst},
            device_id_type=MESH,
        )

    def block(c):
        return pl.ds(c * row_block, row_block)

    scale = HEAD_DIM ** (-0.5) * 1.4426950408889634

    def partner_at(t):
        crossing = jnp.where(t < nz - half, 1, 0)
        side = lax.rem(z // half + crossing, nz // half)
        return side * half + lax.rem(z + t + 1, half)

    def attend(index, carry):
        j = index // nz
        t = lax.rem(index, nz)

        @pl.when(t == 0)
        def _():
            await_bytes(kq_all.at[:, j], landed(0, j))
            for src in range(nz):
                k_rows[pl.ds(src * tok, tok), :] = kq_all[0, j, src].T

        dst = partner_at(t)
        s = jnp.dot(k_rows[...], kq_all[1, j, dst], preferred_element_type=jnp.float32)
        p = jnp.exp2((s - jnp.max(s, axis=0, keepdims=True)) * scale).astype(jnp.bfloat16)

        @pl.when(t == 0)
        def _():
            await_bytes(v_all.at[j, :, pl.ds(0, HEAD_DIM), :], landed(2, j))

        out = jnp.zeros((HEAD_DIM + ONES_ROWS, tok), jnp.float32)
        for src in range(nz):
            out += jnp.dot(
                v_all[j, src], p[src * tok:(src + 1) * tok], preferred_element_type=jnp.float32
            )
        mixed = (out[:HEAD_DIM] / out[HEAD_DIM:HEAD_DIM + 1]).astype(jnp.bfloat16)

        for at in range(nz - 1):

            @pl.when(t == at)
            def _():
                o_send[j, partner(at)] = mixed

                if at >= far:
                    o_copy(j, at, pl.ds(0, tok), j).start()
                else:

                    @pl.when(jnp.logical_not(middle))
                    def _():
                        o_copy(j, at, pl.ds(0, tok), j).start()

                    @pl.when(middle & (j < last))
                    def _():
                        o_copy(j, at, pl.ds(0, tok), local + j).start()

                if at == far - 1:

                    @pl.when(middle & (j == last))
                    def _():
                        for c in range(chunks):
                            for to in reversed(range(far)):
                                o_copy(j, to, block(c), local + last + c).start()

        @pl.when(t == nz - 1)
        def _():
            att_t[j, pl.ds(pl.multiple_of(slot(z, z) * HEAD_DIM, 16), HEAD_DIM), :] = mixed

        @pl.when((j == 0) & (t == nz - 1))
        def _():
            await_bytes(text_all.at[b, pl.ds(0, nz - 1)], text_rsem)
            for r in range(1, nb):
                wide_copy(r).start()

        return carry

    lax.fori_loop(0, local * nz, attend, 0)

    for copy in loads:
        copy.wait()
    await_bytes(w_v, w_sem)
    rows = lax.broadcasted_iota(jnp.int32, (nb, LANES), 0)
    lanes = lax.broadcasted_iota(jnp.int32, (nb, LANES), 1)
    matching = jnp.zeros((nb, LANES), jnp.int32)
    for i in range(nb):
        matching = jnp.where(rows == i, labels_ref[i], matching)
    match_out[...] = matching
    depth = nz * HEAD_DIM

    def product(j, first, count, at):
        return jnp.dot(
            att_t[j, pl.ds(first * HEAD_DIM, count * HEAD_DIM), at].T,
            w_v[pl.ds(j * depth + first * HEAD_DIM, count * HEAD_DIM), :],
            preferred_element_type=jnp.float32,
        )

    halves = [pl.ds(at, tok // 2) for at in range(0, tok, tok // 2)]
    for j in range(local):
        if nz > 2:
            await_bytes(att_t.at[j, pl.ds(0, (nz - 2) * HEAD_DIM)], o_rsem.at[j])
        for here in halves:
            old = res_v[here, :].astype(jnp.float32) if j == 0 else acc[here, :]
            acc[here, :] = old + product(j, 0, nz - 1, here)
    for j in range(last):
        await_bytes(att_t.at[j, pl.ds(0, HEAD_DIM)], o_rsem.at[local + j])
        for here in halves:
            acc[here, :] += product(j, nz - 1, 1, here)
    await_bytes(text_all.at[pl.ds(0, nb - 1)], wide_rsem)

    def hid_copy(c):
        return pltpu.make_async_copy(hid_v.at[block(c), :], hid_out.at[0, block(c), :], hid_sem)

    pool = jnp.zeros((1, features), jnp.float32)
    for c in range(chunks):
        here = block(c)
        await_bytes(att_t.at[last, pl.ds(0, HEAD_DIM), here], o_rsem.at[local + last + c])
        summed = acc[here, :] + product(last, nz - 1, 1, here)
        hid_v[here, :] = summed.astype(jnp.bfloat16)
        if c < chunks - 1:
            hid_copy(c).start()
        centred = summed - jnp.mean(summed, axis=-1, keepdims=True)
        variance = jnp.mean(centred * centred, axis=-1, keepdims=True)
        pool += jnp.sum(centred * lax.rsqrt(variance + 1e-05), axis=0, keepdims=True)

    pool_all[z] = pool * gain_ref[...].reshape(1, features)

    def pool_copy(t):
        return pltpu.make_async_remote_copy(
            src_ref=pool_all.at[z],
            dst_ref=pool_all.at[z],
            send_sem=pool_ssem,
            recv_sem=pool_rsem,
            device_id={"seq": partner(t)},
            device_id_type=MESH,
        )

    for t in range(nz - 1):
        pool_copy(t).start()
    hid_copy(chunks - 1).start()
    await_bytes(pool_all.at[pl.ds(0, nz - 1)], pool_rsem)
    pooled = pool_all[0]
    for src in range(1, nz):
        pooled = pooled + pool_all[src]
    pooled = pooled / (nz * tok)

    high = pooled.astype(jnp.bfloat16).astype(jnp.float32)
    middle = (pooled - high).astype(jnp.bfloat16).astype(jnp.float32)
    low = pooled - high - middle
    row_id = lax.broadcasted_iota(jnp.int32, (16, features), 0)
    parts = jnp.where(
        row_id == 0, high, jnp.where(row_id == 1, middle, jnp.where(row_id == 2, low, 0.0))
    ).astype(jnp.bfloat16)
    embed = jnp.sum(
        jnp.dot(parts, wproj_v[...], preferred_element_type=jnp.float32), axis=0, keepdims=True
    )
    products = jnp.zeros((nb, 1), jnp.float32)
    for src in range(nz):
        texts = text_all[:, src].reshape(nb, cols)
        products += jnp.sum(
            texts * embed[:, src * cols:(src + 1) * cols], axis=1, keepdims=True
        )
    squares = jnp.sum(embed * embed, axis=1, keepdims=True)
    row = jnp.sum(jnp.where(rows == lanes, products, 0.0), axis=0, keepdims=True)
    row_all[b] = jnp.where(lanes[:1] == nb, squares, row)

    def row_copy(r):
        return pltpu.make_async_remote_copy(
            src_ref=row_all.at[b],
            dst_ref=row_all.at[b],
            send_sem=row_ssem,
            recv_sem=row_rsem,
            device_id={"batch": lax.rem(b + r, nb)},
            device_id_type=MESH,
        )

    for r in range(1, nb):
        row_copy(r).start()

    await_bytes(kq_all.at[:, :, pl.ds(0, nz - 1)], move_send.at[0])
    await_bytes(o_send.at[:, pl.ds(0, nz - 1)], move_send.at[1])
    await_bytes(o_send.at[:, pl.ds(0, nz - 1)], o_ssem)
    await_bytes(text_all.at[b, pl.ds(0, nz - 1)], text_ssem)
    await_bytes(text_all.at[pl.ds(0, nb - 1)], wide_ssem)
    await_bytes(pool_all.at[pl.ds(0, nz - 1)], pool_ssem)
    pltpu.make_async_copy(hid_v, hid_out.at[0], hid_sem).wait()
    await_bytes(row_all.at[pl.ds(0, nb - 1)], row_rsem)
    row_out[...] = row_all[...].reshape(nb, LANES)
    await_bytes(row_all.at[pl.ds(0, nb - 1)], row_ssem)


def loss_kernel(
    nb, hid_ref, row_ref, match_ref, hid_out, img_out, txt_out, img_ref, txt_ref, hid_sem, loss_sem
):
    store = pltpu.make_async_copy(hid_ref, hid_out, hid_sem)
    store.start()
    b = lax.axis_index("batch")
    rows = lax.broadcasted_iota(jnp.int32, (nb, LANES), 0)
    lanes = lax.broadcasted_iota(jnp.int32, (nb, LANES), 1)
    total = row_ref[...]
    norm = jnp.sum(jnp.where(lanes == nb, total, 0.0), axis=1, keepdims=True)
    logits = total * lax.rsqrt(norm + 1e-06)
    valid = lanes < nb
    picked = jnp.where(match_ref[...] == lanes, logits, 0.0)
    shown = jnp.where(valid, logits, -3e38)
    top = jnp.max(shown, axis=1, keepdims=True)
    image = (
        top
        + jnp.log(jnp.sum(jnp.where(valid, jnp.exp(shown - top), 0.0), axis=1, keepdims=True))
        - jnp.sum(jnp.where(valid, picked, 0.0), axis=1, keepdims=True)
    )
    peak = jnp.max(logits, axis=0, keepdims=True)
    text = (
        peak
        + jnp.log(jnp.sum(jnp.exp(logits - peak), axis=0, keepdims=True))
        - jnp.sum(picked, axis=0, keepdims=True)
    )
    img_ref[0] = jnp.sum(jnp.where((rows == b) & (lanes == 0), image, 0.0))
    txt_ref[0] = jnp.sum(jnp.where((rows == 0) & (lanes == b), text, 0.0))
    image_store = pltpu.make_async_copy(img_ref, img_out, loss_sem.at[0])
    text_store = pltpu.make_async_copy(txt_ref, txt_out, loss_sem.at[1])
    image_store.start()
    text_store.start()
    store.wait()
    image_store.wait()
    text_store.wait()


def fused(queries, keys, values, residual_in, w_out, ln_gain, w_proj, texts, labels):
    nb, nz = lax.axis_size("batch"), lax.axis_size("seq")
    _, tok, features = queries.shape
    local = HEADS // nz
    chunks = tok // min(128, tok)
    cols = texts.shape[1]
    bf16, f32 = jnp.bfloat16, jnp.float32
    anywhere = pl.BlockSpec(memory_space=pl.ANY)
    dma = pltpu.SemaphoreType.DMA
    wide = pltpu.VMEM((tok, features), bf16)
    tall = pltpu.VMEM((features, tok), bf16)
    hidden_shape = jax.ShapeDtypeStruct((1, tok, features), bf16)
    loss_shape = jax.ShapeDtypeStruct((1,), f32)
    hbm, vmem = pl.BlockSpec(memory_space=pltpu.HBM), pl.BlockSpec(memory_space=pltpu.VMEM)
    hidden, rows, matching = pl.pallas_call(
        functools.partial(fused_kernel, nb, nz),
        out_shape=(
            hidden_shape,
            jax.ShapeDtypeStruct((nb, LANES), f32),
            jax.ShapeDtypeStruct((nb, LANES), jnp.int32),
        ),
        in_specs=[hbm] * 9,
        out_specs=(anywhere, vmem, vmem),
        scratch_shapes=[
            pltpu.VMEM((3, tok, features), bf16), tall, tall, tall,
            pltpu.VMEM((2, local, nz, HEAD_DIM, tok), bf16),
            pltpu.VMEM((local, nz, HEAD_DIM + ONES_ROWS, tok), bf16),
            pltpu.VMEM((nz * tok, HEAD_DIM), bf16),
            pltpu.VMEM((features,), f32),
            pltpu.VMEM((1, cols), f32),
            pltpu.SMEM(labels.shape, jnp.int32),
            pltpu.VMEM((local, nz, HEAD_DIM, tok), bf16),
            pltpu.VMEM((local, nz * HEAD_DIM, tok), bf16),
            pltpu.VMEM((features, features), bf16),
            wide,
            pltpu.VMEM((tok, features), f32),
            wide,
            pltpu.VMEM(w_proj.shape, bf16),
            pltpu.VMEM((nb, nz, 1, cols), f32),
            pltpu.VMEM((nz, 1, features), f32),
            pltpu.VMEM((nb, 1, LANES), f32),
            dma((2 + local,)), dma((5,)), dma,
            dma((2,)), dma((2 * local,)),
            dma, dma((2 * local - 1 + chunks,)),
            dma, dma, dma, dma, dma, dma, dma, dma, dma,
        ],
        compiler_params=pltpu.CompilerParams(
            collective_id=0, has_side_effects=True, vmem_limit_bytes=40 * 1024 * 1024
        ),
    )(
        *(pltpu.with_memory_space_constraint(x, pltpu.HBM) for x in (queries, keys, values, residual_in, w_out, ln_gain, w_proj,
        texts, labels))
    )
    return pl.pallas_call(
        functools.partial(loss_kernel, nb),
        out_shape=(hidden_shape, loss_shape, loss_shape),
        in_specs=[anywhere, vmem, vmem],
        out_specs=(hbm, hbm, hbm),
        scratch_shapes=[pltpu.SMEM((1,), f32), pltpu.SMEM((1,), f32), dma, dma((2,))],
        compiler_params=pltpu.CompilerParams(vmem_limit_bytes=4 * 1024 * 1024),
    )(hidden, rows, matching)


def row_lse(logits, axis):
    maxima = jnp.max(logits, axis=axis, keepdims=True)
    return jnp.squeeze(maxima, axis) + jnp.log(jnp.sum(jnp.exp(logits - maxima), axis=axis))


def body(queries, keys, values, residual_in, w_out, ln_gain, w_proj, texts, labels):
    seq_count = lax.axis_size("seq")
    images_here, tok_rows, features = queries.shape
    head_count = HEADS // seq_count
    head_cols = head_count * HEAD_DIM
    score_scale = HEAD_DIM ** (-0.5)
    query_all = lax.all_to_all(queries, "seq", split_axis=2, concat_axis=1, tiled=True)
    key_all = lax.all_to_all(keys, "seq", split_axis=2, concat_axis=1, tiled=True)
    value_all = lax.all_to_all(values, "seq", split_axis=2, concat_axis=1, tiled=True)
    items = query_all.shape[0]
    length = query_all.shape[1]
    block_rows = min(512, length)
    query_heads = query_all.reshape(items, length, head_count, HEAD_DIM)
    key_heads = key_all.reshape(items, length, head_count, HEAD_DIM)
    value_heads = value_all.reshape(items, length, head_count, HEAD_DIM)

    def one_block(offset):
        query_block = lax.dynamic_slice_in_dim(query_heads, offset, block_rows, 1)
        scores = (
            jnp.einsum(
                "nqhd,nkhd->nhqk", query_block, key_heads, preferred_element_type=jnp.float32
            )
            * score_scale
        )
        maxima = jnp.max(scores, axis=-1, keepdims=True)
        weights = jnp.exp(scores - maxima)
        weights = (weights / jnp.sum(weights, axis=-1, keepdims=True)).astype(jnp.bfloat16)
        mixed = jnp.einsum(
            "nhqk,nkhd->nqhd", weights, value_heads, preferred_element_type=jnp.float32
        )
        return mixed.astype(jnp.bfloat16).reshape(items, block_rows, head_cols)

    offsets = jnp.arange(length // block_rows) * block_rows
    blocks = lax.map(one_block, offsets)
    attended = jnp.moveaxis(blocks, 0, 1).reshape(items, length, head_cols)
    attended = lax.all_to_all(attended, "seq", split_axis=1, concat_axis=2, tiled=True)
    mixed_out = jnp.dot(attended.reshape(-1, features), w_out, preferred_element_type=jnp.float32)
    summed = residual_in.astype(jnp.float32) + mixed_out.reshape(images_here, tok_rows, features)
    hidden_out = summed.astype(jnp.bfloat16)
    centred = summed - jnp.mean(summed, axis=-1, keepdims=True)
    variance = jnp.mean(centred * centred, axis=-1, keepdims=True)
    normed = centred * lax.rsqrt(variance + 1e-05) * ln_gain
    pool_part = jnp.sum(normed, axis=1) / (tok_rows * seq_count)
    embed_cols = EMBED // seq_count
    pooled = lax.psum(pool_part, "seq")
    embedding = jnp.dot(pooled, w_proj.astype(jnp.float32), precision=lax.Precision.HIGHEST)
    inverse = lax.rsqrt(jnp.sum(embedding * embedding, axis=1) + 1e-06)
    unit_rows = embedding * inverse[:, None]
    embed_piece = lax.dynamic_slice_in_dim(
        unit_rows, lax.axis_index("seq") * embed_cols, embed_cols, 1
    )
    gathered, text_all = (
        lax.all_gather(embed_piece, "batch", axis=0, tiled=True),
        lax.all_gather(texts, "batch", axis=0, tiled=True),
    )
    logit_part = jnp.dot(gathered, text_all.T, precision=lax.Precision.HIGHEST)
    logits = lax.psum(logit_part, "seq")
    matched = labels[:, None] == jnp.arange(logits.shape[1], dtype=jnp.int32)[None, :]
    picked = jnp.where(matched, logits, jnp.float32(0.0))
    image_all = row_lse(logits, 1) - jnp.sum(picked, axis=1)
    text_every = row_lse(logits, 0) - jnp.sum(picked, axis=0)
    first_row = lax.axis_index("batch") * images_here
    image_loss = lax.dynamic_slice_in_dim(image_all, first_row, images_here, 0)
    text_loss = lax.dynamic_slice_in_dim(text_every, first_row, images_here, 0)
    return (hidden_out, image_loss, text_loss)


def program(queries, keys, values, residual_in, w_out, ln_gain, w_proj, texts, labels):
    nb, nz = lax.axis_size("batch"), lax.axis_size("seq")
    fits = (
        queries.shape[0] == 1
        and texts.shape[0] == 1
        and HEADS % nz == 0
        and nz % 2 == 0
        and HEADS * HEAD_DIM % LANES == 0
        and queries.shape[1] % 128 == 0
        and queries.shape[1] <= 512
        and queries.shape[1] * nz <= 2048
        and texts.shape[1] % LANES == 0
        and nb % 8 == 0
        and nb < LANES
    )
    chosen = fused if fits else body
    return chosen(queries, keys, values, residual_in, w_out, ln_gain, w_proj, texts, labels)


def solution(mesh):
    in_specs = (
        P("batch", "seq", None),
        P("batch", "seq", None),
        P("batch", "seq", None),
        P("batch", "seq", None),
        P(),
        P(),
        P(),
        P("batch", "seq"),
        P(),
    )
    out_specs = (P("batch", "seq", None), P("batch"), P("batch"))
    return jax.shard_map(program, mesh=mesh, in_specs=in_specs, out_specs=out_specs, check_vma=False)
```

```python
import functools

import jax
import jax.numpy as jnp
from jax import lax
from jax.experimental import pallas as pl
from jax.experimental.pallas import tpu as pltpu
from jax.sharding import PartitionSpec as P

HEADS = 16
HEAD_DIM = 80
EMBED = 1024
LANES = 128
ONES_ROWS = 16
MESH = pl.DeviceIdType.MESH


def fused_kernel(
    nb, nz,
    q_hbm, k_hbm, v_hbm, res_hbm, w_hbm, gain_hbm, wproj_hbm, texts_hbm, labels_hbm,
    hid_out, row_out, match_out,
    inputs, k_t, q_t, v_t, kq_all, v_all, k_rows,
    gain_ref, texts_ref, labels_ref, o_send, att_t, w_v, res_v, acc, hid_v, wproj_v, text_all, pool_send, pool_all, row_all,
    in_sem, load_sem, w_sem, move_send, move_recv, o_ssem, o_rsem,
    text_ssem, text_rsem, wide_ssem, wide_rsem, pool_ssem, pool_rsem, row_ssem, row_rsem, hid_sem,
):
    b = lax.axis_index("batch")
    z = lax.axis_index("seq")
    _, tok, features = inputs.shape
    local = HEADS // nz
    cols = texts_ref.shape[1]
    half = max(1, nz // 2)
    ends = [-(-(j + 1) * nz * HEAD_DIM // LANES) * LANES for j in range(local)]
    groups = list(zip([0] + ends[:-1], ends))

    def partner(t):
        side = lax.rem(z // half + (1 if t < nz - half else 0), nz // half)
        return side * half + lax.rem(z + t + 1, half)

    barrier = pltpu.get_barrier_semaphore()
    sources, turned = (k_hbm, q_hbm, v_hbm), (k_t, q_t, v_t)

    def columns(j):
        return pl.ds(groups[j][0], groups[j][1] - groups[j][0])

    def in_copy(arr, j):
        return pltpu.make_async_copy(
            sources[arr].at[0, :, columns(j)],
            inputs.at[arr, :, columns(j)],
            in_sem.at[arr if j == 0 else 2 + j],
        )

    for t in range(nz - 1):
        pl.semaphore_signal(
            barrier, inc=1, device_id={"seq": partner(t)}, device_id_type=MESH
        )
    for j in range(local):
        for arr in range(3):
            in_copy(arr, j).start()
    for r in range(1, nb):
        pl.semaphore_signal(
            barrier, inc=1, device_id={"batch": lax.rem(b + r, nb)}, device_id_type=MESH
        )
    odd = lax.rem(b, 2)
    for t in range(nz - 1):
        pl.semaphore_signal(
            barrier,
            inc=1,
            device_id={"batch": b + 1 - 2 * odd, "seq": partner(t)},
            device_id_type=MESH,
        )
    loads = [
        pltpu.make_async_copy(src, dst, load_sem.at[i])
        for i, (src, dst) in enumerate(
            (
                (res_hbm.at[0], res_v), (wproj_hbm, wproj_v), (gain_hbm, gain_ref),
                (labels_hbm, labels_ref),
            )
        )
    ]
    w_rows = []
    for j in range(local):
        for at in range(nz):
            across = lax.rem(at + half, nz)
            src = jnp.where(z < half, nz - 1 - across, across)
            start = pl.multiple_of((j * nz + src) * HEAD_DIM, 16)
            w_rows.append(
                pltpu.make_async_copy(
                    w_hbm.at[pl.ds(start, HEAD_DIM)],
                    w_v.at[pl.ds((j * nz + at) * HEAD_DIM, HEAD_DIM)],
                    w_sem,
                )
            )
    text_load = pltpu.make_async_copy(texts_hbm, texts_ref, load_sem.at[4])
    text_load.start()
    for copy in loads + w_rows:
        copy.start()

    v_all[:, :, pl.ds(HEAD_DIM, ONES_ROWS), :] = jnp.ones(
        (local, nz, ONES_ROWS, tok), jnp.bfloat16
    )

    def await_bytes(ref, sem):
        pltpu.make_async_copy(ref, ref, sem).wait()

    def turn(arr, j):
        if j == 0:
            in_copy(arr, j).wait()
        elif arr == 0:
            await_bytes(inputs.at[:, :, columns(j)], in_sem.at[2 + j])
        for at in range(groups[j][0], groups[j][1], LANES):
            turned[arr][pl.ds(at, LANES), :] = inputs[arr, :, pl.ds(at, LANES)].T

    def piece(arr, j, src):
        if arr == 2:
            return v_all.at[j, src, pl.ds(0, HEAD_DIM), :]
        return kq_all.at[arr, j, src]

    def landed(arr, j):
        return move_recv.at[local + j if arr == 2 else j]

    def rows_of(arr, j, dst):
        at = pl.multiple_of((j * nz + dst) * HEAD_DIM, 16)
        return turned[arr].at[pl.ds(at, HEAD_DIM), :]

    def remote(arr, j, t):
        dst = partner(t)
        return pltpu.make_async_remote_copy(
            src_ref=rows_of(arr, j, dst),
            dst_ref=piece(arr, j, z),
            send_sem=move_send.at[arr // 2],
            recv_sem=landed(arr, j),
            device_id={"seq": dst},
            device_id_type=MESH,
        )

    def send_piece(arr, j):
        for t in range(nz - 1):
            remote(arr, j, t).start()
        pltpu.make_async_copy(rows_of(arr, j, z), piece(arr, j, z), landed(arr, j)).start()

    def text_copy(t):
        return pltpu.make_async_remote_copy(
            src_ref=texts_ref,
            dst_ref=text_all.at[b, z],
            send_sem=text_ssem,
            recv_sem=text_rsem,
            device_id={"seq": partner(t)},
            device_id_type=MESH,
        )

    def wide_copy(r):
        return pltpu.make_async_remote_copy(
            src_ref=text_all.at[b],
            dst_ref=text_all.at[b],
            send_sem=wide_ssem,
            recv_sem=wide_rsem,
            device_id={"batch": lax.rem(b + r, nb)},
            device_id_type=MESH,
        )

    for j in range(local):
        for arr in range(3):
            turn(arr, j)
            if j == arr == 0:
                pl.semaphore_wait(barrier, 2 * (nz - 1) + nb - 1)
            send_piece(arr, j)
            if j == arr == 0:
                text_load.wait()
                for t in range(nz - 1):
                    text_copy(t).start()
                text_all[b, z] = texts_ref[...]

    row_block = min(128, tok)
    chunks = tok // row_block

    far = nz - half
    last = local - 1
    middle = (z == half - 1) | (z == half)

    def slot(src, dst):
        return lax.rem(jnp.where(dst < half, nz - 1 - src, src) + half, nz)

    def o_copy(j, t, at, sem):
        dst = partner(t)
        rows = pl.ds(pl.multiple_of(slot(z, dst) * HEAD_DIM, 16), HEAD_DIM)
        return pltpu.make_async_remote_copy(
            src_ref=o_send.at[j, dst, :, at],
            dst_ref=att_t.at[j, rows, at],
            send_sem=o_ssem,
            recv_sem=o_rsem.at[sem],
            device_id={"seq": dst},
            device_id_type=MESH,
        )

    def block(c):
        return pl.ds(c * row_block, row_block)

    scale = HEAD_DIM ** (-0.5) * 1.4426950408889634

    def partner_at(t):
        crossing = jnp.where(t < nz - half, 1, 0)
        side = lax.rem(z // half + crossing, nz // half)
        return side * half + lax.rem(z + t + 1, half)

    def attend(index, carry):
        j = index // nz
        t = lax.rem(index, nz)

        @pl.when(t == 0)
        def _():
            await_bytes(kq_all.at[:, j], landed(0, j))
            for src in range(nz):
                k_rows[pl.ds(src * tok, tok), :] = kq_all[0, j, src].T

        dst = partner_at(t)
        s = jnp.dot(k_rows[...], kq_all[1, j, dst], preferred_element_type=jnp.float32)
        p = jnp.exp2((s - jnp.max(s, axis=0, keepdims=True)) * scale).astype(jnp.bfloat16)

        @pl.when(t == 0)
        def _():
            await_bytes(v_all.at[j, :, pl.ds(0, HEAD_DIM), :], landed(2, j))

        out = jnp.zeros((HEAD_DIM + ONES_ROWS, tok), jnp.float32)
        for src in range(nz):
            out += jnp.dot(
                v_all[j, src], p[src * tok:(src + 1) * tok], preferred_element_type=jnp.float32
            )
        mixed = (out[:HEAD_DIM] / out[HEAD_DIM:HEAD_DIM + 1]).astype(jnp.bfloat16)

        for at in range(nz - 1):

            @pl.when(t == at)
            def _():
                o_send[j, partner(at)] = mixed

                if at >= far:
                    o_copy(j, at, pl.ds(0, tok), j).start()
                else:

                    @pl.when(jnp.logical_not(middle))
                    def _():
                        o_copy(j, at, pl.ds(0, tok), j).start()

                    @pl.when(middle & (j < last))
                    def _():
                        o_copy(j, at, pl.ds(0, tok), local + j).start()

                if at == far - 1:

                    @pl.when(middle & (j == last))
                    def _():
                        for c in range(chunks):
                            for to in reversed(range(far)):
                                o_copy(j, to, block(c), local + last + c).start()

        @pl.when(t == nz - 1)
        def _():
            att_t[j, pl.ds(pl.multiple_of(slot(z, z) * HEAD_DIM, 16), HEAD_DIM), :] = mixed

        @pl.when((j == 0) & (t == nz - 1))
        def _():
            await_bytes(text_all.at[b, pl.ds(0, nz - 1)], text_rsem)
            for r in range(1, nb):
                wide_copy(r).start()

        return carry

    lax.fori_loop(0, local * nz, attend, 0)

    for copy in loads:
        copy.wait()
    await_bytes(w_v, w_sem)
    rows = lax.broadcasted_iota(jnp.int32, (nb, LANES), 0)
    lanes = lax.broadcasted_iota(jnp.int32, (nb, LANES), 1)
    matching = jnp.zeros((nb, LANES), jnp.int32)
    for i in range(nb):
        matching = jnp.where(rows == i, labels_ref[i], matching)
    match_out[...] = matching
    depth = nz * HEAD_DIM

    def product(j, first, count, at):
        return jnp.dot(
            att_t[j, pl.ds(first * HEAD_DIM, count * HEAD_DIM), at].T,
            w_v[pl.ds(j * depth + first * HEAD_DIM, count * HEAD_DIM), :],
            preferred_element_type=jnp.float32,
        )

    halves = [pl.ds(at, tok // 2) for at in range(0, tok, tok // 2)]
    for j in range(local):
        if nz > 2:
            await_bytes(att_t.at[j, pl.ds(0, (nz - 2) * HEAD_DIM)], o_rsem.at[j])
        for here in halves:
            old = res_v[here, :].astype(jnp.float32) if j == 0 else acc[here, :]
            acc[here, :] = old + product(j, 0, nz - 1, here)
    for j in range(last):
        await_bytes(att_t.at[j, pl.ds(0, HEAD_DIM)], o_rsem.at[local + j])
        for here in halves:
            acc[here, :] += product(j, nz - 1, 1, here)
    await_bytes(text_all.at[pl.ds(0, nb - 1)], wide_rsem)

    def hid_copy(c):
        return pltpu.make_async_copy(hid_v.at[block(c), :], hid_out.at[0, block(c), :], hid_sem)

    pool = jnp.zeros((1, features), jnp.float32)
    for c in range(chunks):
        here = block(c)
        await_bytes(att_t.at[last, pl.ds(0, HEAD_DIM), here], o_rsem.at[local + last + c])
        summed = acc[here, :] + product(last, nz - 1, 1, here)
        hid_v[here, :] = summed.astype(jnp.bfloat16)
        if c < chunks - 1:
            hid_copy(c).start()
        centred = summed - jnp.mean(summed, axis=-1, keepdims=True)
        variance = jnp.mean(centred * centred, axis=-1, keepdims=True)
        pool += jnp.sum(centred * lax.rsqrt(variance + 1e-05), axis=0, keepdims=True)

    pool_send[...] = pool * gain_ref[...].reshape(1, features)
    head = b + 1 - odd

    def pool_copy(to):
        return pltpu.make_async_remote_copy(
            src_ref=pool_send,
            dst_ref=pool_all.at[odd * nz + z],
            send_sem=pool_ssem,
            recv_sem=pool_rsem,
            device_id={"batch": head, "seq": to},
            device_id_type=MESH,
        )

    for t in range(nz - 1):
        pool_copy(partner(t)).start()

    @pl.when(odd == 0)
    def _():
        pool_copy(z).start()

    hid_copy(chunks - 1).start()

    def row_copy(r):
        pair = pl.ds(b - 1, 2)
        return pltpu.make_async_remote_copy(
            src_ref=row_all.at[pair],
            dst_ref=row_all.at[pair],
            send_sem=row_ssem,
            recv_sem=row_rsem,
            device_id={"batch": lax.rem(b + r, nb)},
            device_id_type=MESH,
        )

    @pl.when(odd == 1)
    def _():
        await_bytes(pool_all.at[pl.ds(0, 2 * nz - 1)], pool_rsem)
        row_id = lax.broadcasted_iota(jnp.int32, (16, features), 0)
        parts = jnp.zeros((16, features), jnp.float32)
        for image in range(2):
            pooled = pool_send[...] if image else pool_all[0]
            for at in range(1, nz):
                src = nz + lax.rem(z + at, nz) if image else at
                pooled = pooled + pool_all[src]
            pooled = pooled / (nz * tok)
            high = pooled.astype(jnp.bfloat16).astype(jnp.float32)
            middle_part = (pooled - high).astype(jnp.bfloat16).astype(jnp.float32)
            low = pooled - high - middle_part
            for place, part in enumerate((high, middle_part, low)):
                parts = jnp.where(row_id == 8 * image + place, part, parts)
        embeds = jnp.dot(
            parts.astype(jnp.bfloat16), wproj_v[...], preferred_element_type=jnp.float32
        )
        for image in range(2):
            embed = jnp.sum(embeds[8 * image:8 * image + 8], axis=0, keepdims=True)
            products = jnp.zeros((nb, 1), jnp.float32)
            for src in range(nz):
                texts = text_all[:, src].reshape(nb, cols)
                products += jnp.sum(
                    texts * embed[:, src * cols:(src + 1) * cols], axis=1, keepdims=True
                )
            squares = jnp.sum(embed * embed, axis=1, keepdims=True)
            row = jnp.sum(jnp.where(rows == lanes, products, 0.0), axis=0, keepdims=True)
            row_all[b - 1 + image] = jnp.where(lanes[:1] == nb, squares, row)
        for r in range(1, nb):
            row_copy(r).start()

    await_bytes(kq_all.at[:, :, pl.ds(0, nz - 1)], move_send.at[0])
    await_bytes(o_send.at[:, pl.ds(0, nz - 1)], move_send.at[1])
    await_bytes(o_send.at[:, pl.ds(0, nz - 1)], o_ssem)
    await_bytes(text_all.at[b, pl.ds(0, nz - 1)], text_ssem)
    await_bytes(text_all.at[pl.ds(0, nb - 1)], wide_ssem)
    pltpu.make_async_copy(hid_v, hid_out.at[0], hid_sem).wait()

    @pl.when(odd == 0)
    def _():
        await_bytes(pool_all.at[pl.ds(0, nz)], pool_ssem)
        await_bytes(row_all.at[pl.ds(0, nb)], row_rsem)

    @pl.when(odd == 1)
    def _():
        await_bytes(pool_all.at[pl.ds(0, nz - 1)], pool_ssem)
        await_bytes(row_all.at[pl.ds(0, nb - 2)], row_rsem)
        await_bytes(row_all.at[pl.ds(0, 2 * (nb - 1))], row_ssem)

    row_out[...] = row_all[pl.ds(0, nb)].reshape(nb, LANES)


def loss_kernel(
    nb, hid_ref, row_ref, match_ref, hid_out, img_out, txt_out, img_ref, txt_ref, hid_sem, loss_sem
):
    store = pltpu.make_async_copy(hid_ref, hid_out, hid_sem)
    store.start()
    b = lax.axis_index("batch")
    rows = lax.broadcasted_iota(jnp.int32, (nb, LANES), 0)
    lanes = lax.broadcasted_iota(jnp.int32, (nb, LANES), 1)
    total = row_ref[...]
    norm = jnp.sum(jnp.where(lanes == nb, total, 0.0), axis=1, keepdims=True)
    logits = total * lax.rsqrt(norm + 1e-06)
    valid = lanes < nb
    picked = jnp.where(match_ref[...] == lanes, logits, 0.0)
    shown = jnp.where(valid, logits, -3e38)
    top = jnp.max(shown, axis=1, keepdims=True)
    image = (
        top
        + jnp.log(jnp.sum(jnp.where(valid, jnp.exp(shown - top), 0.0), axis=1, keepdims=True))
        - jnp.sum(jnp.where(valid, picked, 0.0), axis=1, keepdims=True)
    )
    peak = jnp.max(logits, axis=0, keepdims=True)
    text = (
        peak
        + jnp.log(jnp.sum(jnp.exp(logits - peak), axis=0, keepdims=True))
        - jnp.sum(picked, axis=0, keepdims=True)
    )
    img_ref[0] = jnp.sum(jnp.where((rows == b) & (lanes == 0), image, 0.0))
    txt_ref[0] = jnp.sum(jnp.where((rows == 0) & (lanes == b), text, 0.0))
    image_store = pltpu.make_async_copy(img_ref, img_out, loss_sem.at[0])
    text_store = pltpu.make_async_copy(txt_ref, txt_out, loss_sem.at[1])
    image_store.start()
    text_store.start()
    store.wait()
    image_store.wait()
    text_store.wait()


def fused(queries, keys, values, residual_in, w_out, ln_gain, w_proj, texts, labels):
    nb, nz = lax.axis_size("batch"), lax.axis_size("seq")
    _, tok, features = queries.shape
    local = HEADS // nz
    chunks = tok // min(128, tok)
    cols = texts.shape[1]
    bf16, f32 = jnp.bfloat16, jnp.float32
    anywhere = pl.BlockSpec(memory_space=pl.ANY)
    dma = pltpu.SemaphoreType.DMA
    wide = pltpu.VMEM((tok, features), bf16)
    tall = pltpu.VMEM((features, tok), bf16)
    hidden_shape = jax.ShapeDtypeStruct((1, tok, features), bf16)
    loss_shape = jax.ShapeDtypeStruct((1,), f32)
    hbm, vmem = pl.BlockSpec(memory_space=pltpu.HBM), pl.BlockSpec(memory_space=pltpu.VMEM)
    hidden, rows, matching = pl.pallas_call(
        functools.partial(fused_kernel, nb, nz),
        out_shape=(
            hidden_shape,
            jax.ShapeDtypeStruct((nb, LANES), f32),
            jax.ShapeDtypeStruct((nb, LANES), jnp.int32),
        ),
        in_specs=[hbm] * 9,
        out_specs=(anywhere, vmem, vmem),
        scratch_shapes=[
            pltpu.VMEM((3, tok, features), bf16), tall, tall, tall,
            pltpu.VMEM((2, local, nz, HEAD_DIM, tok), bf16),
            pltpu.VMEM((local, nz, HEAD_DIM + ONES_ROWS, tok), bf16),
            pltpu.VMEM((nz * tok, HEAD_DIM), bf16),
            pltpu.VMEM((features,), f32),
            pltpu.VMEM((1, cols), f32),
            pltpu.SMEM(labels.shape, jnp.int32),
            pltpu.VMEM((local, nz, HEAD_DIM, tok), bf16),
            pltpu.VMEM((local, nz * HEAD_DIM, tok), bf16),
            pltpu.VMEM((features, features), bf16),
            wide,
            pltpu.VMEM((tok, features), f32),
            wide,
            pltpu.VMEM(w_proj.shape, bf16),
            pltpu.VMEM((nb, nz, 1, cols), f32),
            pltpu.VMEM((1, features), f32),
            pltpu.VMEM((2 * nz, 1, features), f32),
            pltpu.VMEM((2 * nb, 1, LANES), f32),
            dma((2 + local,)), dma((5,)), dma,
            dma((2,)), dma((2 * local,)),
            dma, dma((2 * local - 1 + chunks,)),
            dma, dma, dma, dma, dma, dma, dma, dma, dma,
        ],
        compiler_params=pltpu.CompilerParams(
            collective_id=0, has_side_effects=True, vmem_limit_bytes=40 * 1024 * 1024
        ),
    )(
        *(pltpu.with_memory_space_constraint(x, pltpu.HBM) for x in (queries, keys, values, residual_in, w_out, ln_gain, w_proj,
        texts, labels))
    )
    return pl.pallas_call(
        functools.partial(loss_kernel, nb),
        out_shape=(hidden_shape, loss_shape, loss_shape),
        in_specs=[anywhere, vmem, vmem],
        out_specs=(hbm, hbm, hbm),
        scratch_shapes=[pltpu.SMEM((1,), f32), pltpu.SMEM((1,), f32), dma, dma((2,))],
        compiler_params=pltpu.CompilerParams(vmem_limit_bytes=4 * 1024 * 1024),
    )(hidden, rows, matching)


def row_lse(logits, axis):
    maxima = jnp.max(logits, axis=axis, keepdims=True)
    return jnp.squeeze(maxima, axis) + jnp.log(jnp.sum(jnp.exp(logits - maxima), axis=axis))


def body(queries, keys, values, residual_in, w_out, ln_gain, w_proj, texts, labels):
    seq_count = lax.axis_size("seq")
    images_here, tok_rows, features = queries.shape
    head_count = HEADS // seq_count
    head_cols = head_count * HEAD_DIM
    score_scale = HEAD_DIM ** (-0.5)
    query_all = lax.all_to_all(queries, "seq", split_axis=2, concat_axis=1, tiled=True)
    key_all = lax.all_to_all(keys, "seq", split_axis=2, concat_axis=1, tiled=True)
    value_all = lax.all_to_all(values, "seq", split_axis=2, concat_axis=1, tiled=True)
    items = query_all.shape[0]
    length = query_all.shape[1]
    block_rows = min(512, length)
    query_heads = query_all.reshape(items, length, head_count, HEAD_DIM)
    key_heads = key_all.reshape(items, length, head_count, HEAD_DIM)
    value_heads = value_all.reshape(items, length, head_count, HEAD_DIM)

    def one_block(offset):
        query_block = lax.dynamic_slice_in_dim(query_heads, offset, block_rows, 1)
        scores = (
            jnp.einsum(
                "nqhd,nkhd->nhqk", query_block, key_heads, preferred_element_type=jnp.float32
            )
            * score_scale
        )
        maxima = jnp.max(scores, axis=-1, keepdims=True)
        weights = jnp.exp(scores - maxima)
        weights = (weights / jnp.sum(weights, axis=-1, keepdims=True)).astype(jnp.bfloat16)
        mixed = jnp.einsum(
            "nhqk,nkhd->nqhd", weights, value_heads, preferred_element_type=jnp.float32
        )
        return mixed.astype(jnp.bfloat16).reshape(items, block_rows, head_cols)

    offsets = jnp.arange(length // block_rows) * block_rows
    blocks = lax.map(one_block, offsets)
    attended = jnp.moveaxis(blocks, 0, 1).reshape(items, length, head_cols)
    attended = lax.all_to_all(attended, "seq", split_axis=1, concat_axis=2, tiled=True)
    mixed_out = jnp.dot(attended.reshape(-1, features), w_out, preferred_element_type=jnp.float32)
    summed = residual_in.astype(jnp.float32) + mixed_out.reshape(images_here, tok_rows, features)
    hidden_out = summed.astype(jnp.bfloat16)
    centred = summed - jnp.mean(summed, axis=-1, keepdims=True)
    variance = jnp.mean(centred * centred, axis=-1, keepdims=True)
    normed = centred * lax.rsqrt(variance + 1e-05) * ln_gain
    pool_part = jnp.sum(normed, axis=1) / (tok_rows * seq_count)
    embed_cols = EMBED // seq_count
    pooled = lax.psum(pool_part, "seq")
    embedding = jnp.dot(pooled, w_proj.astype(jnp.float32), precision=lax.Precision.HIGHEST)
    inverse = lax.rsqrt(jnp.sum(embedding * embedding, axis=1) + 1e-06)
    unit_rows = embedding * inverse[:, None]
    embed_piece = lax.dynamic_slice_in_dim(
        unit_rows, lax.axis_index("seq") * embed_cols, embed_cols, 1
    )
    gathered, text_all = (
        lax.all_gather(embed_piece, "batch", axis=0, tiled=True),
        lax.all_gather(texts, "batch", axis=0, tiled=True),
    )
    logit_part = jnp.dot(gathered, text_all.T, precision=lax.Precision.HIGHEST)
    logits = lax.psum(logit_part, "seq")
    matched = labels[:, None] == jnp.arange(logits.shape[1], dtype=jnp.int32)[None, :]
    picked = jnp.where(matched, logits, jnp.float32(0.0))
    image_all = row_lse(logits, 1) - jnp.sum(picked, axis=1)
    text_every = row_lse(logits, 0) - jnp.sum(picked, axis=0)
    first_row = lax.axis_index("batch") * images_here
    image_loss = lax.dynamic_slice_in_dim(image_all, first_row, images_here, 0)
    text_loss = lax.dynamic_slice_in_dim(text_every, first_row, images_here, 0)
    return (hidden_out, image_loss, text_loss)


def program(queries, keys, values, residual_in, w_out, ln_gain, w_proj, texts, labels):
    nb, nz = lax.axis_size("batch"), lax.axis_size("seq")
    fits = (
        queries.shape[0] == 1
        and texts.shape[0] == 1
        and HEADS % nz == 0
        and nz % 2 == 0
        and HEADS * HEAD_DIM % LANES == 0
        and queries.shape[1] % 128 == 0
        and queries.shape[1] <= 512
        and queries.shape[1] * nz <= 2048
        and texts.shape[1] % LANES == 0
        and nb % 8 == 0
        and nb < LANES
    )
    chosen = fused if fits else body
    return chosen(queries, keys, values, residual_in, w_out, ln_gain, w_proj, texts, labels)


def solution(mesh):
    in_specs = (
        P("batch", "seq", None),
        P("batch", "seq", None),
        P("batch", "seq", None),
        P("batch", "seq", None),
        P(),
        P(),
        P(),
        P("batch", "seq"),
        P(),
    )
    out_specs = (P("batch", "seq", None), P("batch"), P("batch"))
    return jax.shard_map(program, mesh=mesh, in_specs=in_specs, out_specs=out_specs, check_vma=False)
```
